8 devices in a mesh: replica: 4 (over z, y, x), data: 2 (over core).
Axes of the slice: x: 2, y: 2, z: 1, core: 2. Of those that a mesh axis runs over, the one named last changes fastest.
Arguments:
- x_seq: bfloat16 [256, 16, 1024], P(('replica', 'data'))
- dy_seq: float32 [256, 16, 1024], P(('replica', 'data'))
- w_stack: bfloat16 [6, 2048, 4096], replicated
- b_stack: float32 [6, 4096], replicated
Outputs:
- output 1: float32 [6, 2048, 4096], replicated
- output 2: float32 [6, 4096], replicated
- output 3: float32 [256, 16, 1024], P(('replica', 'data'))
All inputs are finite; a program needn't handle non-finite values.
Results may differ from the reference program's by a relative error of at most 0.0156497.
Values are sent between devices in bfloat16 or wider.
A program may use at most 1.25 GiB of HBM per device.

```python
import jax
import jax.numpy as jnp
from jax import lax

HIDDEN = 1024
LAYERS = 6
BATCH_DEV = 32
SEQ = 16
REPLICA = 4
DATA = 2


def setup_inputs(seed: int = 0) -> dict:
    shards = REPLICA * DATA
    batch_rows = BATCH_DEV * shards
    key_list = jax.random.split(jax.random.key(seed), 4)
    x_seq = jax.random.normal(key_list[0], (batch_rows, SEQ, HIDDEN), jnp.float32).astype(jnp.bfloat16)
    dy_seq = jax.random.normal(key_list[1], (batch_rows, SEQ, HIDDEN), jnp.float32)
    w_scale = 1.5 * (2 * HIDDEN) ** -0.5
    w_stack = (jax.random.normal(key_list[2], (LAYERS, 2 * HIDDEN, 4 * HIDDEN), jnp.float32) * w_scale).astype(jnp.bfloat16)
    gate_shift = jnp.concatenate([jnp.ones((2 * HIDDEN,), jnp.float32), jnp.zeros((HIDDEN,), jnp.float32), jnp.ones((HIDDEN,), jnp.float32)])
    b_stack = gate_shift + 0.5 * jax.random.normal(key_list[3], (LAYERS, 4 * HIDDEN), jnp.float32)
    return {'x_seq': x_seq, 'dy_seq': dy_seq, 'w_stack': w_stack, 'b_stack': b_stack}


def layer_forward(u_seq, w_layer, b_layer):
    batch_rows = u_seq.shape[1]

    def time_step(carry_state, u_step):
        h_prev, c_prev = carry_state
        z_all = jnp.dot(jnp.concatenate([u_step, h_prev], axis=-1), w_layer, preferred_element_type=jnp.float32) + b_layer
        z_i, z_f, z_g, z_o = jnp.split(z_all, 4, axis=-1)
        gate_i = jax.nn.sigmoid(z_i)
        gate_f = jax.nn.sigmoid(z_f)
        gate_g = jnp.tanh(z_g)
        gate_o = jax.nn.sigmoid(z_o)
        c_new = gate_f * c_prev + gate_i * gate_g
        tanh_c = jnp.tanh(c_new)
        h_new = (gate_o * tanh_c).astype(jnp.bfloat16)
        return (h_new, c_new), (h_new, c_new, tanh_c, gate_i, gate_f, gate_g, gate_o)

    init_state = (jnp.zeros((batch_rows, HIDDEN), jnp.bfloat16), jnp.zeros((batch_rows, HIDDEN), jnp.float32))
    return lax.scan(time_step, init_state, u_seq)[1]


def layer_backward(u_seq, w_layer, saved_acts, dh_seq):
    h_seq, c_seq, tanh_seq, i_seq, f_seq, g_seq, o_seq = saved_acts
    h_prev_seq = jnp.concatenate([jnp.zeros_like(h_seq[:1]), h_seq[:-1]], axis=0)
    c_prev_seq = jnp.concatenate([jnp.zeros_like(c_seq[:1]), c_seq[:-1]], axis=0)

    def time_step(carry_state, step_in):
        dh_rec, dc_next = carry_state
        dh_out, c_prev, tanh_c, gate_i, gate_f, gate_g, gate_o = step_in
        dh_tot = dh_out + dh_rec
        dc_cur = dc_next + dh_tot * gate_o * (1.0 - tanh_c * tanh_c)
        dz_all = jnp.concatenate([dc_cur * gate_g * gate_i * (1.0 - gate_i), dc_cur * c_prev * gate_f * (1.0 - gate_f), dc_cur * gate_i * (1.0 - gate_g * gate_g), dh_tot * tanh_c * gate_o * (1.0 - gate_o)], axis=-1)
        dz_low = dz_all.astype(jnp.bfloat16)
        du_all = jnp.dot(dz_low, w_layer.T, preferred_element_type=jnp.float32)
        return (du_all[:, HIDDEN:], dc_cur * gate_f), (dz_low, du_all[:, :HIDDEN], jnp.sum(dz_all, axis=0))

    init_state = (jnp.zeros_like(dh_seq[0]), jnp.zeros_like(dh_seq[0]))
    dz_seq, dx_seq, db_steps = lax.scan(time_step, init_state, (dh_seq, c_prev_seq, tanh_seq, i_seq, f_seq, g_seq, o_seq), reverse=True)[1]
    uh_seq = jnp.concatenate([u_seq, h_prev_seq], axis=-1)
    row_count = uh_seq.shape[0] * uh_seq.shape[1]
    dw_layer = jnp.dot(uh_seq.reshape(row_count, 2 * HIDDEN).T, dz_seq.reshape(row_count, 4 * HIDDEN), preferred_element_type=jnp.float32)
    return dw_layer, jnp.sum(db_steps, axis=0), dx_seq


def shard_grads(x_rows, dy_rows, w_stack, b_stack):
    u_first = jnp.swapaxes(x_rows, 0, 1)

    def fwd_layer(u_seq, layer_in):
        saved_acts = layer_forward(u_seq, layer_in[0], layer_in[1])
        return saved_acts[0], (u_seq, saved_acts)

    layer_inputs, layer_saved = lax.scan(fwd_layer, u_first, (w_stack, b_stack))[1]

    def bwd_layer(dh_seq, layer_in):
        dw_layer, db_layer, dx_seq = layer_backward(layer_in[1], layer_in[0], layer_in[2], dh_seq)
        return dx_seq, (dw_layer, db_layer)

    dx_seq, grads = lax.scan(bwd_layer, jnp.swapaxes(dy_rows, 0, 1), (w_stack, layer_inputs, layer_saved), reverse=True)
    return grads[0], grads[1], jnp.swapaxes(dx_seq, 0, 1)


def reference(x_seq, dy_seq, w_stack, b_stack):
    shards = REPLICA * DATA
    x_parts = x_seq.reshape(shards, BATCH_DEV, SEQ, HIDDEN)
    dy_parts = dy_seq.reshape(shards, BATCH_DEV, SEQ, HIDDEN)

    def add_shard(totals, shard_in):
        dw_all, db_all, dx_rows = shard_grads(shard_in[0], shard_in[1], w_stack, b_stack)
        dw_sum = totals[0] + dw_all.astype(jnp.bfloat16).astype(jnp.float32)
        db_sum = totals[1] + db_all.astype(jnp.bfloat16).astype(jnp.float32)
        return (dw_sum, db_sum), dx_rows

    init_totals = (jnp.zeros(w_stack.shape, jnp.float32), jnp.zeros(b_stack.shape, jnp.float32))
    totals, dx_parts = lax.scan(add_shard, init_totals, (x_parts, dy_parts))
    return totals[0], totals[1], dx_parts.reshape(x_seq.shape)
```

```python
import functools

import jax
import jax.numpy as jnp
from jax import lax
from jax.experimental import pallas as pl
from jax.experimental.pallas import tpu as pltpu
from jax.sharding import PartitionSpec as P

VMEM_LIMIT = 62 * 1024 * 1024
CHIPS = 4
PEERS = 8
EXTRA = 16
NT = (((1,), (1,)), ((), ()))
MESH = pl.DeviceIdType.MESH


def sigmoid(z):
    return 0.5 * jnp.tanh(0.5 * z) + 0.5


def forward_kernel(layer, steps, rows, hidden, u_ref, w_hbm, b_ref, gates_hbm, c_hbm, h_ref, w_in, w_rec, gates, c_buf, w_sem, out_sem):
    tile = 512
    tiles = 4 * hidden // tile

    def in_copy(j):
        cols = pl.ds(j * tile, tile)
        return pltpu.make_async_copy(w_hbm.at[layer, pl.ds(0, hidden), cols], w_in.at[:, cols], w_sem.at[j])

    for j in range(tiles):
        in_copy(j).start()
    rec_copy = pltpu.make_async_copy(w_hbm.at[layer, pl.ds(hidden, hidden)], w_rec, w_sem.at[tiles])
    rec_copy.start()
    for j in range(tiles):
        cols = pl.ds(j * tile, tile)
        in_copy(j).wait()
        gates[:, cols] = jnp.dot(u_ref[...], w_in[:, cols], preferred_element_type=jnp.float32) + b_ref[0, :, cols]
    rec_copy.wait()
    part = 256

    def out_copies(t):
        r = pl.ds(pl.multiple_of(t * rows, rows), rows)
        return (pltpu.make_async_copy(gates.at[r], gates_hbm.at[r], out_sem.at[0]), pltpu.make_async_copy(c_buf.at[r], c_hbm.at[r], out_sem.at[1]))

    def step(t, first):
        r = pl.ds(pl.multiple_of(t * rows, rows), rows)
        if not first:
            rp = pl.ds(pl.multiple_of((t - 1) * rows, rows), rows)
            h_prev = h_ref[rp, :]
            for copy in out_copies(t - 1):
                copy.start()
        for p in range(hidden // part):
            z = []
            for k in range(4):
                cols = pl.ds(k * hidden + p * part, part)
                zk = gates[r, cols]
                if not first:
                    zk = zk + jnp.dot(h_prev, w_rec[:, cols], preferred_element_type=jnp.float32)
                z.append(zk)
            pc = pl.ds(p * part, part)
            gate_i, gate_f, gate_g, gate_o = sigmoid(z[0]), sigmoid(z[1]), jnp.tanh(z[2]), sigmoid(z[3])
            c_new = gate_i * gate_g
            if not first:
                c_new = gate_f * c_buf[rp, pc] + c_new
            for k, v in enumerate((gate_i, gate_f, gate_g, gate_o)):
                gates[r, pl.ds(k * hidden + p * part, part)] = v
            c_buf[r, pc] = c_new
            h_ref[r, pc] = (gate_o * jnp.tanh(c_new)).astype(jnp.bfloat16)

    step(0, True)

    @pl.loop(1, steps)
    def _(t):
        step(t, False)

    for copy in out_copies(steps - 1):
        copy.start()
    pltpu.make_async_copy(gates, gates_hbm, out_sem.at[0]).wait()
    pltpu.make_async_copy(c_buf, c_hbm, out_sem.at[1]).wait()


def forward(layer, u, w_stack, b_stack, steps):
    n, hidden = u.shape
    width = 4 * hidden
    whole = pl.BlockSpec(memory_space=pltpu.VMEM)
    anywhere = pl.BlockSpec(memory_space=pl.ANY)
    return pl.pallas_call(
        functools.partial(forward_kernel, layer, steps, n // steps, hidden),
        grid=(1,),
        in_specs=[
            pl.BlockSpec((n, hidden), lambda i: (0, 0)),
            anywhere,
            pl.BlockSpec((1, 1, width), lambda i: (layer, 0, 0)),
        ],
        out_specs=[anywhere, anywhere, pl.BlockSpec((n, hidden), lambda i: (0, 0))],
        out_shape=[
            jax.ShapeDtypeStruct((n, width), jnp.float32),
            jax.ShapeDtypeStruct((n, hidden), jnp.float32),
            jax.ShapeDtypeStruct((n, hidden), jnp.bfloat16),
        ],
        scratch_shapes=[
            pltpu.VMEM((hidden, width), jnp.bfloat16),
            pltpu.VMEM((hidden, width), jnp.bfloat16),
            pltpu.VMEM((n, width), jnp.float32),
            pltpu.VMEM((n, hidden), jnp.float32),
            pltpu.SemaphoreType.DMA((9,)),
            pltpu.SemaphoreType.DMA((2,)),
        ],
        compiler_params=pltpu.CompilerParams(vmem_limit_bytes=VMEM_LIMIT),
        cost_estimate=pl.CostEstimate(flops=2 * n * 2 * hidden * width * 4, bytes_accessed=2 * 2 * hidden * width, transcendentals=0),
        name="lstm_forward",
    )(u, w_stack, b_stack)


def backward_kernel(layer, steps, rows, hidden, e_ref, gates_ref, c_ref, cp_ref, w_hbm, land, dx_ref, r_buf, dc_buf, db_buf, dz_buf, w_in, w_rec, w_sem, own_sem, send_sem, recv_sem):
    s = pl.program_id(0)
    t = steps - 1 - s
    width = 4 * hidden
    share = width // PEERS
    n = steps * rows
    chip = lax.axis_index("replica")
    core = lax.axis_index("data")
    chips = (chip, chip + 1 - 2 * lax.rem(chip, 2), lax.rem(chip + 2, 4), 3 - chip)
    cores = (core, 1 - core)
    rec_copy = pltpu.make_async_copy(w_hbm.at[layer, pl.ds(hidden, hidden)], w_rec, w_sem.at[0])
    in_copy = pltpu.make_async_copy(w_hbm.at[layer, pl.ds(0, hidden)], w_in, w_sem.at[1])

    def own_copy(start, count):
        r = pl.ds(start, count)
        cols = pl.ds(pl.multiple_of((chip * 2 + core) * share, share), share)
        return pltpu.make_async_copy(dz_buf.at[r, cols], land.at[chip, r], own_sem)

    def send_copy(k, start, count):
        to_chip, to_core = chips[k % 4], cores[k // 4]
        r = pl.ds(start, count)
        cols = pl.ds(pl.multiple_of((to_chip * 2 + to_core) * share, share), share)
        return pltpu.make_async_remote_copy(
            src_ref=dz_buf.at[r, cols],
            dst_ref=land.at[chip + 4 * (k // 4), r],
            send_sem=send_sem.at[k],
            recv_sem=recv_sem.at[k],
            device_id=(to_chip, to_core),
            device_id_type=MESH,
        )

    def send(start, count):
        for k in (3, 7, 1, 2, 5, 6, 4):
            send_copy(k, start, count).start()
        own_copy(start, count).start()

    @pl.when(s == 0)
    def _():
        rec_copy.start()
        in_copy.start()
        barrier = pltpu.get_barrier_semaphore()
        for k in range(1, PEERS):
            pl.semaphore_signal(barrier, inc=1, device_id=(chips[k % 4], cores[k // 4]), device_id_type=MESH)
        r_buf[...] = jnp.zeros_like(r_buf)
        dc_buf[...] = jnp.zeros_like(dc_buf)
        db_buf[...] = jnp.zeros_like(db_buf)
        rec_copy.wait()
        pl.semaphore_wait(barrier, PEERS - 1)

    for q in range(1, 4):
        @pl.when(s == 4 * q)
        def _():
            send(n - 4 * q * rows, 4 * rows)

    @pl.when(s == steps - 1)
    def _():
        send(rows, 3 * rows)

    keep = jnp.where(t == 0, 0.0, 1.0)
    part = 256
    for p in range(hidden // part):
        pc = pl.ds(p * part, part)
        gate_i, gate_f, gate_g, gate_o = (gates_ref[:, pl.ds(k * hidden + p * part, part)] for k in range(4))
        tanh_c = jnp.tanh(c_ref[:, pc])
        c_prev = cp_ref[:, pc] * keep
        dh = e_ref[:, pc] + r_buf[:, pc]
        dc = dc_buf[:, pc] + dh * gate_o * (1.0 - tanh_c * tanh_c)
        dz = (
            dc * gate_g * gate_i * (1.0 - gate_i),
            dc * c_prev * gate_f * (1.0 - gate_f),
            dc * gate_i * (1.0 - gate_g * gate_g),
            dh * tanh_c * gate_o * (1.0 - gate_o),
        )
        dc_buf[:, pc] = dc * gate_f
        for k in range(4):
            cols = pl.ds(k * hidden + p * part, part)
            dz_buf[pl.ds(pl.multiple_of(t * rows, rows), rows), cols] = dz[k].astype(jnp.bfloat16)
            db_buf[:, cols] += jnp.sum(dz[k], axis=0, keepdims=True)

    @pl.when(s < steps - 1)
    def _():
        low = dz_buf[pl.ds(pl.multiple_of(t * rows, rows), rows), :]
        for p in range(hidden // part):
            pc = pl.ds(p * part, part)
            r_buf[:, pc] = lax.dot_general(low, w_rec[pc, :], NT, preferred_element_type=jnp.float32)

    @pl.when(s == steps - 1)
    def _():
        dz_buf[pl.ds(n, EXTRA), :] = jnp.broadcast_to(db_buf[...], (EXTRA, width)).astype(jnp.bfloat16)
        in_copy.wait()

        def dx_tile(p):
            pc = pl.ds(pl.multiple_of(p * part, part), part)
            dx_ref[:, pc] = lax.dot_general(dz_buf[pl.ds(0, n), :], w_in[pc, :], NT, preferred_element_type=jnp.float32)

        @pl.loop(0, 1)
        def _(p):
            dx_tile(p)

        send(0, rows)
        send(n, EXTRA)

        @pl.loop(1, hidden // part)
        def _(p):
            dx_tile(p)

        own_copy(0, n + EXTRA).wait()
        for k in range(1, PEERS):
            send_copy(k, 0, n + EXTRA).wait_send()
            cols = pl.ds(pl.multiple_of((chip * 2 + core) * share, share), share)
            pltpu.make_async_remote_copy(
                src_ref=dz_buf.at[:, cols],
                dst_ref=land.at[chips[k % 4] + 4 * (k // 4)],
                send_sem=send_sem.at[k],
                recv_sem=recv_sem.at[k],
                device_id=(chips[k % 4], cores[k // 4]),
                device_id_type=MESH,
            ).wait_recv()


def backward(layer, e_seq, gates, c_seq, w_stack, steps):
    n, hidden = e_seq.shape
    width = 4 * hidden
    rows = n // steps
    last = steps - 1
    anywhere = pl.BlockSpec(memory_space=pl.ANY)
    return pl.pallas_call(
        functools.partial(backward_kernel, layer, steps, rows, hidden),
        grid=(steps,),
        in_specs=[
            pl.BlockSpec((rows, hidden), lambda s: (last - s, 0)),
            pl.BlockSpec((rows, width), lambda s: (last - s, 0)),
            pl.BlockSpec((rows, hidden), lambda s: (last - s, 0)),
            pl.BlockSpec((rows, hidden), lambda s: (jnp.maximum(last - 1 - s, 0), 0)),
            anywhere,
        ],
        out_specs=[anywhere, pl.BlockSpec((n, hidden), lambda s: (0, 0))],
        out_shape=[
            jax.ShapeDtypeStruct((PEERS, n + EXTRA, width // PEERS), jnp.bfloat16),
            jax.ShapeDtypeStruct((n, hidden), jnp.float32),
        ],
        scratch_shapes=[
            pltpu.VMEM((rows, hidden), jnp.float32),
            pltpu.VMEM((rows, hidden), jnp.float32),
            pltpu.VMEM((1, width), jnp.float32),
            pltpu.VMEM((n + EXTRA, width), jnp.bfloat16),
            pltpu.VMEM((hidden, width), jnp.bfloat16),
            pltpu.VMEM((hidden, width), jnp.bfloat16),
            pltpu.SemaphoreType.DMA((2,)),
            pltpu.SemaphoreType.DMA,
            pltpu.SemaphoreType.DMA((PEERS,)),
            pltpu.SemaphoreType.DMA((PEERS,)),
        ],
        compiler_params=pltpu.CompilerParams(vmem_limit_bytes=VMEM_LIMIT, collective_id=layer, has_side_effects=True),
        cost_estimate=pl.CostEstimate(flops=2 * n * 2 * hidden * width * 4, bytes_accessed=2 * 2 * hidden * width, transcendentals=0),
        name="lstm_backward",
    )(e_seq, gates, c_seq, c_seq, w_stack)


def weight_kernel(n, rows, hidden, land_ref, u_own, u_other, h_own, h_other, out_ref, acc, db_acc, dz_t, dz_shift):
    s = pl.program_id(0)
    share = land_ref.shape[-1]

    @pl.when(s == 0)
    def _():
        acc[...] = jnp.zeros_like(acc)
        db_acc[...] = jnp.zeros_like(db_acc)

    db_acc[...] += land_ref[0, pl.ds(n, EXTRA), :].astype(jnp.float32)
    dz_t[...] = land_ref[0, pl.ds(0, n), :].T
    dz_shift[...] = jnp.concatenate([land_ref[0, pl.ds(rows, n - rows), :], jnp.zeros((rows, share), jnp.bfloat16)], axis=0).T
    part = 256

    def add(u_ref, h_ref):
        @pl.loop(0, hidden // part)
        def _(p):
            for base, lhs, rhs in ((0, dz_t, u_ref), (hidden, dz_shift, h_ref)):
                cols = pl.ds(pl.multiple_of(base + p * part, part), part)
                rc = pl.ds(pl.multiple_of(p * part, part), part)
                dw = jnp.dot(lhs[...], rhs[0, :, rc], preferred_element_type=jnp.float32)
                acc[:, cols] += dw.astype(jnp.bfloat16).astype(jnp.float32)

    @pl.when(s < CHIPS)
    def _():
        add(u_own, h_own)

    @pl.when(s >= CHIPS)
    def _():
        add(u_other, h_other)

    @pl.when(s == PEERS - 1)
    def _():
        @pl.loop(0, 2 * hidden // part)
        def _(p):
            cols = pl.ds(pl.multiple_of(p * part, part), part)
            out_ref[cols, :] = acc[:, cols].T.astype(jnp.bfloat16)

        out_ref[pl.ds(2 * hidden, EXTRA), :] = db_acc[...].astype(jnp.bfloat16)


def weight_gradient(land, u_all, h_all, rows):
    _, height, share = land.shape
    _, n, hidden = u_all[0].shape
    own = pl.BlockSpec((1, n, hidden), lambda s: (jnp.minimum(s, CHIPS - 1), 0, 0))
    other = pl.BlockSpec((1, n, hidden), lambda s: (jnp.maximum(s - CHIPS, 0), 0, 0))
    return pl.pallas_call(
        functools.partial(weight_kernel, n, rows, hidden),
        grid=(PEERS,),
        in_specs=[pl.BlockSpec((1, height, share), lambda s: (s, 0, 0)), own, other, own, other],
        out_specs=pl.BlockSpec((2 * hidden + EXTRA, share), lambda s: (0, 0)),
        out_shape=jax.ShapeDtypeStruct((2 * hidden + EXTRA, share), jnp.bfloat16),
        scratch_shapes=[
            pltpu.VMEM((share, 2 * hidden), jnp.float32),
            pltpu.VMEM((EXTRA, share), jnp.float32),
            pltpu.VMEM((share, n), jnp.bfloat16),
            pltpu.VMEM((share, n), jnp.bfloat16),
        ],
        compiler_params=pltpu.CompilerParams(vmem_limit_bytes=VMEM_LIMIT),
        cost_estimate=pl.CostEstimate(flops=2 * PEERS * n * share * 2 * hidden * 4, bytes_accessed=4 * PEERS * n * hidden, transcendentals=0),
        name="weight_gradient",
    )(land, *u_all, *h_all)


def cast_kernel(core_ref, own_ref, other_ref, own_db, other_db, *refs):
    out_ref, db_ref = refs[-2:]
    core = core_ref[0]
    share = own_ref.shape[-1]
    for chip in range(CHIPS):
        for which, src, src_db in ((core, own_ref, own_db), (1 - core, other_ref, other_db)):
            cols = pl.ds(pl.multiple_of((chip * 2 + which) * share, share), share)
            out_ref[0, :, cols] = src[chip].astype(jnp.float32)
            db_ref[0, :, cols] = src_db[chip, pl.ds(0, 8), :][0:1].astype(jnp.float32)


def cast_into(bufs, core, parts, layer, layers):
    own, other = parts
    _, height, share = own.shape
    height -= EXTRA
    tile = 128
    width = PEERS * share
    big = pl.BlockSpec((CHIPS, tile, share), lambda i: (0, i, 0))
    small = pl.BlockSpec((CHIPS, EXTRA, share), lambda i: (0, height // EXTRA, 0))
    return pl.pallas_call(
        cast_kernel,
        grid=(height // tile,),
        in_specs=[pl.BlockSpec(memory_space=pltpu.SMEM), big, big, small, small] + [pl.BlockSpec(memory_space=pl.ANY)] * len(bufs),
        out_specs=[pl.BlockSpec((1, tile, width), lambda i: (layer, i, 0)), pl.BlockSpec((1, 1, width), lambda i: (layer, 0, 0))],
        out_shape=[jax.ShapeDtypeStruct((layers, height, width), jnp.float32), jax.ShapeDtypeStruct((layers, 1, width), jnp.float32)],
        input_output_aliases={5: 0, 6: 1} if bufs else {},
        compiler_params=pltpu.CompilerParams(vmem_limit_bytes=VMEM_LIMIT),
        cost_estimate=pl.CostEstimate(flops=height * width * 100, bytes_accessed=6 * height * width, transcendentals=0),
        name="cast_gradient",
    )(core, own, other, own, other, *bufs)


def solution(mesh):
    batch_axes = ('replica', 'data')
    swap = [(0, 1), (1, 0)]

    def gather(part):
        own = lax.all_gather(part, 'replica')
        return own, lax.ppermute(own, 'data', swap)

    def local_grads(x_loc, dy_loc, w_stack, b_stack):
        layers = w_stack.shape[0]
        rows, steps, hidden = x_loc.shape
        n = rows * steps
        core = lax.axis_index('data').astype(jnp.int32).reshape(1)
        u = jnp.swapaxes(x_loc, 0, 1).reshape(n, hidden)
        b_rows = b_stack[:, None, :]
        gathered = [gather(u)]
        saved = []
        for layer in range(layers):
            gates, c_seq, u = forward(layer, u, w_stack, b_rows, steps)
            saved.append((gates, c_seq))
            gathered.append(gather(u))
        e_seq = jnp.swapaxes(dy_loc, 0, 1).reshape(n, hidden)
        bufs = ()
        pending = None
        for layer in reversed(range(layers)):
            land, e_seq = backward(layer, e_seq, *saved[layer], w_stack, steps)
            part = weight_gradient(land, gathered[layer], gathered[layer + 1], rows)
            part, e_seq = lax.optimization_barrier((part, e_seq))
            if pending is not None:
                part, pending = lax.optimization_barrier((part, pending))
            parts = gather(part)
            if pending is not None:
                bufs = cast_into(bufs, core, pending, layer + 1, layers)
            pending = parts
        dw, db = cast_into(bufs, core, pending, 0, layers)
        return dw, db.reshape(layers, 4 * hidden), jnp.swapaxes(e_seq.reshape(steps, rows, hidden), 0, 1)

    return jax.shard_map(local_grads, mesh=mesh, in_specs=(P(batch_axes), P(batch_axes), P(), P()), out_specs=(P(), P(), P(batch_axes)), check_vma=False)
```

```python
import functools

import jax
import jax.numpy as jnp
from jax import lax
from jax.experimental import pallas as pl
from jax.experimental.pallas import tpu as pltpu
from jax.sharding import PartitionSpec as P

VMEM_LIMIT = 62 * 1024 * 1024
CHIPS = 4
PEERS = 8
EXTRA = 16
NT = (((1,), (1,)), ((), ()))
MESH = pl.DeviceIdType.MESH


def sigmoid(z):
    return 0.5 * jnp.tanh(0.5 * z) + 0.5


def forward_kernel(layer, steps, rows, hidden, u_ref, w_hbm, b_ref, gates_hbm, c_hbm, h_ref, w_in, w_rec, gates, c_buf, w_sem, out_sem):
    tile = 512
    tiles = 4 * hidden // tile

    def in_copy(j):
        cols = pl.ds(j * tile, tile)
        return pltpu.make_async_copy(w_hbm.at[layer, pl.ds(0, hidden), cols], w_in.at[:, cols], w_sem.at[j])

    for j in range(tiles):
        in_copy(j).start()
    rec_copy = pltpu.make_async_copy(w_hbm.at[layer, pl.ds(hidden, hidden)], w_rec, w_sem.at[tiles])
    rec_copy.start()
    for j in range(tiles):
        cols = pl.ds(j * tile, tile)
        in_copy(j).wait()
        gates[:, cols] = jnp.dot(u_ref[...], w_in[:, cols], preferred_element_type=jnp.float32) + b_ref[0, :, cols]
    rec_copy.wait()
    part = 256

    def out_copies(t):
        r = pl.ds(pl.multiple_of(t * rows, rows), rows)
        return (pltpu.make_async_copy(gates.at[r], gates_hbm.at[r], out_sem.at[0]), pltpu.make_async_copy(c_buf.at[r], c_hbm.at[r], out_sem.at[1]))

    def step(t, first):
        r = pl.ds(pl.multiple_of(t * rows, rows), rows)
        if not first:
            rp = pl.ds(pl.multiple_of((t - 1) * rows, rows), rows)
            h_prev = h_ref[rp, :]
            for copy in out_copies(t - 1):
                copy.start()
        for p in range(hidden // part):
            z = []
            for k in range(4):
                cols = pl.ds(k * hidden + p * part, part)
                zk = gates[r, cols]
                if not first:
                    zk = zk + jnp.dot(h_prev, w_rec[:, cols], preferred_element_type=jnp.float32)
                z.append(zk)
            pc = pl.ds(p * part, part)
            gate_i, gate_f, gate_g, gate_o = sigmoid(z[0]), sigmoid(z[1]), jnp.tanh(z[2]), sigmoid(z[3])
            c_new = gate_i * gate_g
            if not first:
                c_new = gate_f * c_buf[rp, pc] + c_new
            for k, v in enumerate((gate_i, gate_f, gate_g, gate_o)):
                gates[r, pl.ds(k * hidden + p * part, part)] = v
            c_buf[r, pc] = c_new
            h_ref[r, pc] = (gate_o * jnp.tanh(c_new)).astype(jnp.bfloat16)

    step(0, True)

    @pl.loop(1, steps)
    def _(t):
        step(t, False)

    for copy in out_copies(steps - 1):
        copy.start()
    pltpu.make_async_copy(gates, gates_hbm, out_sem.at[0]).wait()
    pltpu.make_async_copy(c_buf, c_hbm, out_sem.at[1]).wait()


def forward(layer, u, w_stack, b_stack, steps):
    n, hidden = u.shape
    width = 4 * hidden
    whole = pl.BlockSpec(memory_space=pltpu.VMEM)
    anywhere = pl.BlockSpec(memory_space=pl.ANY)
    return pl.pallas_call(
        functools.partial(forward_kernel, layer, steps, n // steps, hidden),
        grid=(1,),
        in_specs=[
            pl.BlockSpec((n, hidden), lambda i: (0, 0)),
            anywhere,
            pl.BlockSpec((1, 1, width), lambda i: (layer, 0, 0)),
        ],
        out_specs=[anywhere, anywhere, pl.BlockSpec((n, hidden), lambda i: (0, 0))],
        out_shape=[
            jax.ShapeDtypeStruct((n, width), jnp.float32),
            jax.ShapeDtypeStruct((n, hidden), jnp.float32),
            jax.ShapeDtypeStruct((n, hidden), jnp.bfloat16),
        ],
        scratch_shapes=[
            pltpu.VMEM((hidden, width), jnp.bfloat16),
            pltpu.VMEM((hidden, width), jnp.bfloat16),
            pltpu.VMEM((n, width), jnp.float32),
            pltpu.VMEM((n, hidden), jnp.float32),
            pltpu.SemaphoreType.DMA((9,)),
            pltpu.SemaphoreType.DMA((2,)),
        ],
        compiler_params=pltpu.CompilerParams(vmem_limit_bytes=VMEM_LIMIT),
        cost_estimate=pl.CostEstimate(flops=2 * n * 2 * hidden * width * 4, bytes_accessed=2 * 2 * hidden * width, transcendentals=0),
        name="lstm_forward",
    )(u, w_stack, b_stack)


def backward_kernel(layer, steps, rows, hidden, e_ref, gates_ref, c_ref, cp_ref, w_hbm, token_ref, land, dx_ref, r_buf, dc_buf, db_buf, dz_buf, w_in, w_rec, w_sem, own_sem, send_sem, recv_sem):
    s = pl.program_id(0)
    t = steps - 1 - s
    width = 4 * hidden
    share = width // PEERS
    n = steps * rows
    chip = lax.axis_index("replica")
    core = lax.axis_index("data")
    chips = (chip, chip + 1 - 2 * lax.rem(chip, 2), lax.rem(chip + 2, 4), 3 - chip)
    cores = (core, 1 - core)
    rec_copy = pltpu.make_async_copy(w_hbm.at[layer, pl.ds(hidden, hidden)], w_rec, w_sem.at[0])
    in_copy = pltpu.make_async_copy(w_hbm.at[layer, pl.ds(0, hidden)], w_in, w_sem.at[1])

    def own_copy(start, count):
        r = pl.ds(start, count)
        cols = pl.ds(pl.multiple_of((chip * 2 + core) * share, share), share)
        return pltpu.make_async_copy(dz_buf.at[r, cols], land.at[chip, r], own_sem)

    def send_copy(k, start, count):
        to_chip, to_core = chips[k % 4], cores[k // 4]
        r = pl.ds(start, count)
        cols = pl.ds(pl.multiple_of((to_chip * 2 + to_core) * share, share), share)
        return pltpu.make_async_remote_copy(
            src_ref=dz_buf.at[r, cols],
            dst_ref=land.at[chip + 4 * (k // 4), r],
            send_sem=send_sem.at[k],
            recv_sem=recv_sem.at[k],
            device_id=(to_chip, to_core),
            device_id_type=MESH,
        )

    def send(start, count):
        for k in (3, 7, 1, 2, 5, 6, 4):
            send_copy(k, start, count).start()
        own_copy(start, count).start()

    @pl.when(s == 0)
    def _():
        rec_copy.start()
        in_copy.start()
        barrier = pltpu.get_barrier_semaphore()
        for k in range(1, PEERS):
            pl.semaphore_signal(barrier, inc=1, device_id=(chips[k % 4], cores[k // 4]), device_id_type=MESH)
        r_buf[...] = jnp.zeros_like(r_buf)
        dc_buf[...] = jnp.zeros_like(dc_buf)
        db_buf[...] = jnp.zeros_like(db_buf)
        rec_copy.wait()
        pl.semaphore_wait(barrier, PEERS - 1)

    for q in range(1, 4):
        @pl.when(s == 4 * q)
        def _():
            send(n - 4 * q * rows, 4 * rows)

    @pl.when(s == steps - 1)
    def _():
        send(rows, 3 * rows)

    keep = jnp.where(t == 0, 0.0, 1.0)
    part = 256
    for p in range(hidden // part):
        pc = pl.ds(p * part, part)
        gate_i, gate_f, gate_g, gate_o = (gates_ref[:, pl.ds(k * hidden + p * part, part)] for k in range(4))
        tanh_c = jnp.tanh(c_ref[:, pc])
        c_prev = cp_ref[:, pc] * keep
        dh = e_ref[:, pc] + r_buf[:, pc]
        dc = dc_buf[:, pc] + dh * gate_o * (1.0 - tanh_c * tanh_c)
        dz = (
            dc * gate_g * gate_i * (1.0 - gate_i),
            dc * c_prev * gate_f * (1.0 - gate_f),
            dc * gate_i * (1.0 - gate_g * gate_g),
            dh * tanh_c * gate_o * (1.0 - gate_o),
        )
        dc_buf[:, pc] = dc * gate_f
        for k in range(4):
            cols = pl.ds(k * hidden + p * part, part)
            dz_buf[pl.ds(pl.multiple_of(t * rows, rows), rows), cols] = dz[k].astype(jnp.bfloat16)
            db_buf[:, cols] += jnp.sum(dz[k], axis=0, keepdims=True)

    @pl.when(s < steps - 1)
    def _():
        low = dz_buf[pl.ds(pl.multiple_of(t * rows, rows), rows), :]
        for p in range(hidden // part):
            pc = pl.ds(p * part, part)
            r_buf[:, pc] = lax.dot_general(low, w_rec[pc, :], NT, preferred_element_type=jnp.float32)

    @pl.when(s == steps - 1)
    def _():
        dz_buf[pl.ds(n, EXTRA), :] = jnp.broadcast_to(db_buf[...], (EXTRA, width)).astype(jnp.bfloat16)
        in_copy.wait()

        def dx_tile(p):
            pc = pl.ds(pl.multiple_of(p * part, part), part)
            dx_ref[:, pc] = lax.dot_general(dz_buf[pl.ds(0, n), :], w_in[pc, :], NT, preferred_element_type=jnp.float32)

        @pl.loop(0, 1)
        def _(p):
            dx_tile(p)

        send(0, rows)
        send(n, EXTRA)

        @pl.loop(1, hidden // part)
        def _(p):
            dx_tile(p)

        own_copy(0, n + EXTRA).wait()
        for k in range(1, PEERS):
            send_copy(k, 0, n + EXTRA).wait_send()
            cols = pl.ds(pl.multiple_of((chip * 2 + core) * share, share), share)
            pltpu.make_async_remote_copy(
                src_ref=dz_buf.at[:, cols],
                dst_ref=land.at[chips[k % 4] + 4 * (k // 4)],
                send_sem=send_sem.at[k],
                recv_sem=recv_sem.at[k],
                device_id=(chips[k % 4], cores[k // 4]),
                device_id_type=MESH,
            ).wait_recv()


def backward(layer, e_seq, gates, c_seq, w_stack, token, steps):
    n, hidden = e_seq.shape
    width = 4 * hidden
    rows = n // steps
    last = steps - 1
    anywhere = pl.BlockSpec(memory_space=pl.ANY)
    return pl.pallas_call(
        functools.partial(backward_kernel, layer, steps, rows, hidden),
        grid=(steps,),
        in_specs=[
            pl.BlockSpec((rows, hidden), lambda s: (last - s, 0)),
            pl.BlockSpec((rows, width), lambda s: (last - s, 0)),
            pl.BlockSpec((rows, hidden), lambda s: (last - s, 0)),
            pl.BlockSpec((rows, hidden), lambda s: (jnp.maximum(last - 1 - s, 0), 0)),
            anywhere,
            anywhere,
        ],
        out_specs=[anywhere, pl.BlockSpec((n, hidden), lambda s: (0, 0))],
        out_shape=[
            jax.ShapeDtypeStruct((PEERS, n + EXTRA, width // PEERS), jnp.bfloat16),
            jax.ShapeDtypeStruct((n, hidden), jnp.float32),
        ],
        scratch_shapes=[
            pltpu.VMEM((rows, hidden), jnp.float32),
            pltpu.VMEM((rows, hidden), jnp.float32),
            pltpu.VMEM((1, width), jnp.float32),
            pltpu.VMEM((n + EXTRA, width), jnp.bfloat16),
            pltpu.VMEM((hidden, width), jnp.bfloat16),
            pltpu.VMEM((hidden, width), jnp.bfloat16),
            pltpu.SemaphoreType.DMA((2,)),
            pltpu.SemaphoreType.DMA,
            pltpu.SemaphoreType.DMA((PEERS,)),
            pltpu.SemaphoreType.DMA((PEERS,)),
        ],
        compiler_params=pltpu.CompilerParams(vmem_limit_bytes=VMEM_LIMIT, collective_id=layer, has_side_effects=True),
        cost_estimate=pl.CostEstimate(flops=2 * n * 2 * hidden * width * 4, bytes_accessed=2 * 2 * hidden * width, transcendentals=0),
        name="lstm_backward",
    )(e_seq, gates, c_seq, c_seq, w_stack, token)


def weight_kernel(n, rows, hidden, land_ref, u_own, u_other, h_own, h_other, out_ref, acc, db_acc, dz_t, dz_shift):
    s = pl.program_id(0)
    share = land_ref.shape[-1]

    @pl.when(s == 0)
    def _():
        acc[...] = jnp.zeros_like(acc)
        db_acc[...] = jnp.zeros_like(db_acc)

    db_acc[...] += land_ref[0, pl.ds(n, EXTRA), :].astype(jnp.float32)
    dz_t[...] = land_ref[0, pl.ds(0, n), :].T
    dz_shift[...] = jnp.concatenate([land_ref[0, pl.ds(rows, n - rows), :], jnp.zeros((rows, share), jnp.bfloat16)], axis=0).T
    part = 256

    def add(u_ref, h_ref):
        @pl.loop(0, hidden // part)
        def _(p):
            for base, lhs, rhs in ((0, dz_t, u_ref), (hidden, dz_shift, h_ref)):
                cols = pl.ds(pl.multiple_of(base + p * part, part), part)
                rc = pl.ds(pl.multiple_of(p * part, part), part)
                dw = jnp.dot(lhs[...], rhs[0, :, rc], preferred_element_type=jnp.float32)
                acc[:, cols] += dw.astype(jnp.bfloat16).astype(jnp.float32)

    @pl.when(s < CHIPS)
    def _():
        add(u_own, h_own)

    @pl.when(s >= CHIPS)
    def _():
        add(u_other, h_other)

    @pl.when(s == PEERS - 1)
    def _():
        @pl.loop(0, 2 * hidden // part)
        def _(p):
            cols = pl.ds(pl.multiple_of(p * part, part), part)
            out_ref[cols, :] = acc[:, cols].T.astype(jnp.bfloat16)

        out_ref[pl.ds(2 * hidden, EXTRA), :] = db_acc[...].astype(jnp.bfloat16)


def weight_gradient(land, u_all, h_all, rows):
    _, height, share = land.shape
    _, n, hidden = u_all[0].shape
    own = pl.BlockSpec((1, n, hidden), lambda s: (jnp.minimum(s, CHIPS - 1), 0, 0))
    other = pl.BlockSpec((1, n, hidden), lambda s: (jnp.maximum(s - CHIPS, 0), 0, 0))
    return pl.pallas_call(
        functools.partial(weight_kernel, n, rows, hidden),
        grid=(PEERS,),
        in_specs=[pl.BlockSpec((1, height, share), lambda s: (s, 0, 0)), own, other, own, other],
        out_specs=pl.BlockSpec((2 * hidden + EXTRA, share), lambda s: (0, 0)),
        out_shape=jax.ShapeDtypeStruct((2 * hidden + EXTRA, share), jnp.bfloat16),
        scratch_shapes=[
            pltpu.VMEM((share, 2 * hidden), jnp.float32),
            pltpu.VMEM((EXTRA, share), jnp.float32),
            pltpu.VMEM((share, n), jnp.bfloat16),
            pltpu.VMEM((share, n), jnp.bfloat16),
        ],
        compiler_params=pltpu.CompilerParams(vmem_limit_bytes=VMEM_LIMIT),
        cost_estimate=pl.CostEstimate(flops=2 * PEERS * n * share * 2 * hidden * 4, bytes_accessed=4 * PEERS * n * hidden, transcendentals=0),
        name="weight_gradient",
    )(land, *u_all, *h_all)


def cast_kernel(core_ref, own_ref, other_ref, own_db, other_db, *refs):
    out_ref, db_ref, token_ref = refs[-3:]
    token_ref[...] = jnp.zeros_like(token_ref)
    core = core_ref[0]
    share = own_ref.shape[-1]
    for chip in range(CHIPS):
        for which, src, src_db in ((core, own_ref, own_db), (1 - core, other_ref, other_db)):
            cols = pl.ds(pl.multiple_of((chip * 2 + which) * share, share), share)
            out_ref[0, :, cols] = src[chip].astype(jnp.float32)
            db_ref[0, :, cols] = src_db[chip, pl.ds(0, 8), :][0:1].astype(jnp.float32)


def cast_into(bufs, core, parts, layer, layers):
    own, other = parts
    _, height, share = own.shape
    height -= EXTRA
    tile = 128
    width = PEERS * share
    big = pl.BlockSpec((CHIPS, tile, share), lambda i: (0, i, 0))
    small = pl.BlockSpec((CHIPS, EXTRA, share), lambda i: (0, height // EXTRA, 0))
    return pl.pallas_call(
        cast_kernel,
        grid=(height // tile,),
        in_specs=[pl.BlockSpec(memory_space=pltpu.SMEM), big, big, small, small] + [pl.BlockSpec(memory_space=pl.ANY)] * len(bufs),
        out_specs=[pl.BlockSpec((1, tile, width), lambda i: (layer, i, 0)), pl.BlockSpec((1, 1, width), lambda i: (layer, 0, 0)), pl.BlockSpec((8, 128), lambda i: (0, 0))],
        out_shape=[
            jax.ShapeDtypeStruct((layers, height, width), jnp.float32),
            jax.ShapeDtypeStruct((layers, 1, width), jnp.float32),
            jax.ShapeDtypeStruct((8, 128), jnp.float32),
        ],
        input_output_aliases={5: 0, 6: 1} if bufs else {},
        compiler_params=pltpu.CompilerParams(vmem_limit_bytes=VMEM_LIMIT),
        cost_estimate=pl.CostEstimate(flops=height * width * 100, bytes_accessed=6 * height * width, transcendentals=0),
        name="cast_gradient",
    )(core, own, other, own, other, *bufs)


def solution(mesh):
    batch_axes = ('replica', 'data')
    swap = [(0, 1), (1, 0)]

    def tie(*values):
        return lax.optimization_barrier(values)

    def local_grads(x_loc, dy_loc, w_stack, b_stack):
        layers = w_stack.shape[0]
        rows, steps, hidden = x_loc.shape
        n = rows * steps
        core = lax.axis_index('data').astype(jnp.int32).reshape(1)
        u = jnp.swapaxes(x_loc, 0, 1).reshape(n, hidden)
        b_rows = b_stack[:, None, :]
        own = []
        other = []
        saved = []
        for layer in range(layers):
            own.append(lax.all_gather(u, 'replica'))
            if layer >= 2:
                u, own[layer - 2] = tie(u, own[layer - 2])
                other.append(lax.ppermute(own[layer - 2], 'data', swap))
            if layer >= 3:
                u, other[layer - 3] = tie(u, other[layer - 3])
            gates, c_seq, u = forward(layer, u, w_stack, b_rows, steps)
            saved.append((gates, c_seq))
        own.append(lax.all_gather(u, 'replica'))
        e_seq = jnp.swapaxes(dy_loc, 0, 1).reshape(n, hidden)
        e_seq, own[layers - 2], other[layers - 3] = tie(e_seq, own[layers - 2], other[layers - 3])
        other.append(lax.ppermute(own[layers - 2], 'data', swap))
        bufs = ()
        tokens = {}
        start = jnp.zeros((8, 128), jnp.float32)
        shard_own = None
        for layer in reversed(range(layers)):
            token = tokens.get(layer + 3, start)
            land, e_seq = backward(layer, e_seq, *saved[layer], w_stack, token, steps)
            if layer == layers - 1:
                land, own[layers - 1], own[layers] = tie(land, own[layers - 1], own[layers])
                other.append(lax.ppermute(own[layers - 1], 'data', swap))
                other.append(lax.ppermute(own[layers], 'data', swap))
            part = weight_gradient(land, (own[layer], other[layer]), (own[layer + 1], other[layer + 1]), rows)
            part, e_seq = tie(part, e_seq)
            if shard_own is not None:
                part, shard_own = tie(part, shard_own)
            next_own = lax.all_gather(part, 'replica')
            if shard_own is not None:
                shard_other = lax.ppermute(shard_own, 'data', swap)
                *bufs, tokens[layer + 1] = cast_into(bufs, core, (shard_own, shard_other), layer + 1, layers)
            shard_own = next_own
        shard_own, bufs[1] = tie(shard_own, bufs[1])
        shard_other = lax.ppermute(shard_own, 'data', swap)
        dw, db, _ = cast_into(bufs, core, (shard_own, shard_other), 0, layers)
        return dw, db.reshape(layers, 4 * hidden), jnp.swapaxes(e_seq.reshape(steps, rows, hidden), 0, 1)

    return jax.shard_map(local_grads, mesh=mesh, in_specs=(P(batch_axes), P(batch_axes), P(), P()), out_specs=(P(), P(), P(batch_axes)), check_vma=False)
```

```python
import functools

import jax
import jax.numpy as jnp
from jax import lax
from jax.experimental import pallas as pl
from jax.experimental.pallas import tpu as pltpu
from jax.sharding import PartitionSpec as P

VMEM_LIMIT = 62 * 1024 * 1024
CHIPS = 4
PEERS = 8
EXTRA = 16
NT = (((1,), (1,)), ((), ()))
MESH = pl.DeviceIdType.MESH


def sigmoid(z):
    return 0.5 * jnp.tanh(0.5 * z) + 0.5


def forward_kernel(layer, steps, rows, hidden, u_ref, w_hbm, b_ref, gates_hbm, c_hbm, h_ref, w_in, w_rec, gates, c_buf, w_sem, out_sem):
    tile = 512
    tiles = 4 * hidden // tile

    def in_copy(j):
        cols = pl.ds(j * tile, tile)
        return pltpu.make_async_copy(w_hbm.at[layer, pl.ds(0, hidden), cols], w_in.at[:, cols], w_sem.at[j])

    for j in range(tiles):
        in_copy(j).start()
    rec_copy = pltpu.make_async_copy(w_hbm.at[layer, pl.ds(hidden, hidden)], w_rec, w_sem.at[tiles])
    rec_copy.start()
    for j in range(tiles):
        cols = pl.ds(j * tile, tile)
        in_copy(j).wait()
        gates[:, cols] = jnp.dot(u_ref[...], w_in[:, cols], preferred_element_type=jnp.float32) + b_ref[0, :, cols]
    rec_copy.wait()
    part = 256

    def out_copies(t):
        r = pl.ds(pl.multiple_of(t * rows, rows), rows)
        return (pltpu.make_async_copy(gates.at[r], gates_hbm.at[r], out_sem.at[0]), pltpu.make_async_copy(c_buf.at[r], c_hbm.at[r], out_sem.at[1]))

    def step(t, first):
        r = pl.ds(pl.multiple_of(t * rows, rows), rows)
        if not first:
            rp = pl.ds(pl.multiple_of((t - 1) * rows, rows), rows)
            h_prev = h_ref[rp, :]
            for copy in out_copies(t - 1):
                copy.start()
        for p in range(hidden // part):
            z = []
            for k in range(4):
                cols = pl.ds(k * hidden + p * part, part)
                zk = gates[r, cols]
                if not first:
                    zk = zk + jnp.dot(h_prev, w_rec[:, cols], preferred_element_type=jnp.float32)
                z.append(zk)
            pc = pl.ds(p * part, part)
            gate_i, gate_f, gate_g, gate_o = sigmoid(z[0]), sigmoid(z[1]), jnp.tanh(z[2]), sigmoid(z[3])
            c_new = gate_i * gate_g
            if not first:
                c_new = gate_f * c_buf[rp, pc] + c_new
            for k, v in enumerate((gate_i, gate_f, gate_g, gate_o)):
                gates[r, pl.ds(k * hidden + p * part, part)] = v
            c_buf[r, pc] = c_new
            h_ref[r, pc] = (gate_o * jnp.tanh(c_new)).astype(jnp.bfloat16)

    step(0, True)

    @pl.loop(1, steps)
    def _(t):
        step(t, False)

    for copy in out_copies(steps - 1):
        copy.start()
    pltpu.make_async_copy(gates, gates_hbm, out_sem.at[0]).wait()
    pltpu.make_async_copy(c_buf, c_hbm, out_sem.at[1]).wait()


def forward(layer, u, w_stack, b_stack, steps):
    n, hidden = u.shape
    width = 4 * hidden
    whole = pl.BlockSpec(memory_space=pltpu.VMEM)
    anywhere = pl.BlockSpec(memory_space=pl.ANY)
    return pl.pallas_call(
        functools.partial(forward_kernel, layer, steps, n // steps, hidden),
        grid=(1,),
        in_specs=[
            pl.BlockSpec((n, hidden), lambda i: (0, 0)),
            anywhere,
            pl.BlockSpec((1, 1, width), lambda i: (layer, 0, 0)),
        ],
        out_specs=[anywhere, anywhere, pl.BlockSpec((n, hidden), lambda i: (0, 0))],
        out_shape=[
            jax.ShapeDtypeStruct((n, width), jnp.float32),
            jax.ShapeDtypeStruct((n, hidden), jnp.float32),
            jax.ShapeDtypeStruct((n, hidden), jnp.bfloat16),
        ],
        scratch_shapes=[
            pltpu.VMEM((hidden, width), jnp.bfloat16),
            pltpu.VMEM((hidden, width), jnp.bfloat16),
            pltpu.VMEM((n, width), jnp.float32),
            pltpu.VMEM((n, hidden), jnp.float32),
            pltpu.SemaphoreType.DMA((9,)),
            pltpu.SemaphoreType.DMA((2,)),
        ],
        compiler_params=pltpu.CompilerParams(vmem_limit_bytes=VMEM_LIMIT),
        cost_estimate=pl.CostEstimate(flops=2 * n * 2 * hidden * width * 4, bytes_accessed=2 * 2 * hidden * width, transcendentals=0),
        name="lstm_forward",
    )(u, w_stack, b_stack)


def backward_kernel(layer, steps, rows, hidden, e_ref, gates_ref, c_ref, cp_ref, w_hbm, land, dx_ref, r_buf, dc_buf, db_buf, dz_buf, w_in, w_rec, w_sem, own_sem, send_sem, recv_sem):
    s = pl.program_id(0)
    t = steps - 1 - s
    width = 4 * hidden
    share = width // PEERS
    n = steps * rows
    chip = lax.axis_index("replica")
    core = lax.axis_index("data")
    chips = (chip, chip + 1 - 2 * lax.rem(chip, 2), lax.rem(chip + 2, 4), 3 - chip)
    cores = (core, 1 - core)
    rec_copy = pltpu.make_async_copy(w_hbm.at[layer, pl.ds(hidden, hidden)], w_rec, w_sem.at[0])
    in_copy = pltpu.make_async_copy(w_hbm.at[layer, pl.ds(0, hidden)], w_in, w_sem.at[1])

    def own_copy(start, count):
        r = pl.ds(start, count)
        cols = pl.ds(pl.multiple_of((chip * 2 + core) * share, share), share)
        return pltpu.make_async_copy(dz_buf.at[r, cols], land.at[chip, r], own_sem)

    def send_copy(k, start, count):
        to_chip, to_core = chips[k % 4], cores[k // 4]
        r = pl.ds(start, count)
        cols = pl.ds(pl.multiple_of((to_chip * 2 + to_core) * share, share), share)
        return pltpu.make_async_remote_copy(
            src_ref=dz_buf.at[r, cols],
            dst_ref=land.at[chip + 4 * (k // 4), r],
            send_sem=send_sem.at[k],
            recv_sem=recv_sem.at[k],
            device_id=(to_chip, to_core),
            device_id_type=MESH,
        )

    def send(start, count):
        for k in (3, 7, 1, 2, 5, 6, 4):
            send_copy(k, start, count).start()
        own_copy(start, count).start()

    @pl.when(s == 0)
    def _():
        rec_copy.start()
        in_copy.start()
        barrier = pltpu.get_barrier_semaphore()
        for k in range(1, PEERS):
            pl.semaphore_signal(barrier, inc=1, device_id=(chips[k % 4], cores[k // 4]), device_id_type=MESH)
        r_buf[...] = jnp.zeros_like(r_buf)
        dc_buf[...] = jnp.zeros_like(dc_buf)
        db_buf[...] = jnp.zeros_like(db_buf)
        rec_copy.wait()
        pl.semaphore_wait(barrier, PEERS - 1)

    for q in range(1, 4):
        @pl.when(s == 4 * q)
        def _():
            send(n - 4 * q * rows, 4 * rows)

    @pl.when(s == steps - 1)
    def _():
        send(rows, 3 * rows)

    keep = jnp.where(t == 0, 0.0, 1.0)
    part = 256
    for p in range(hidden // part):
        pc = pl.ds(p * part, part)
        gate_i, gate_f, gate_g, gate_o = (gates_ref[:, pl.ds(k * hidden + p * part, part)] for k in range(4))
        tanh_c = jnp.tanh(c_ref[:, pc])
        c_prev = cp_ref[:, pc] * keep
        dh = e_ref[:, pc] + r_buf[:, pc]
        dc = dc_buf[:, pc] + dh * gate_o * (1.0 - tanh_c * tanh_c)
        dz = (
            dc * gate_g * gate_i * (1.0 - gate_i),
            dc * c_prev * gate_f * (1.0 - gate_f),
            dc * gate_i * (1.0 - gate_g * gate_g),
            dh * tanh_c * gate_o * (1.0 - gate_o),
        )
        dc_buf[:, pc] = dc * gate_f
        for k in range(4):
            cols = pl.ds(k * hidden + p * part, part)
            dz_buf[pl.ds(pl.multiple_of(t * rows, rows), rows), cols] = dz[k].astype(jnp.bfloat16)
            db_buf[:, cols] += jnp.sum(dz[k], axis=0, keepdims=True)

    @pl.when(s < steps - 1)
    def _():
        low = dz_buf[pl.ds(pl.multiple_of(t * rows, rows), rows), :]
        for p in range(hidden // part):
            pc = pl.ds(p * part, part)
            r_buf[:, pc] = lax.dot_general(low, w_rec[pc, :], NT, preferred_element_type=jnp.float32)

    @pl.when(s == steps - 1)
    def _():
        dz_buf[pl.ds(n, EXTRA), :] = jnp.broadcast_to(db_buf[...], (EXTRA, width)).astype(jnp.bfloat16)
        in_copy.wait()

        def dx_tile(p):
            pc = pl.ds(pl.multiple_of(p * part, part), part)
            dx_ref[:, pc] = lax.dot_general(dz_buf[pl.ds(0, n), :], w_in[pc, :], NT, preferred_element_type=jnp.float32)

        @pl.loop(0, 1)
        def _(p):
            dx_tile(p)

        send(0, rows)
        send(n, EXTRA)

        @pl.loop(1, hidden // part)
        def _(p):
            dx_tile(p)

        own_copy(0, n + EXTRA).wait()
        for k in range(1, PEERS):
            send_copy(k, 0, n + EXTRA).wait_send()
            cols = pl.ds(pl.multiple_of((chip * 2 + core) * share, share), share)
            pltpu.make_async_remote_copy(
                src_ref=dz_buf.at[:, cols],
                dst_ref=land.at[chips[k % 4] + 4 * (k // 4)],
                send_sem=send_sem.at[k],
                recv_sem=recv_sem.at[k],
                device_id=(chips[k % 4], cores[k // 4]),
                device_id_type=MESH,
            ).wait_recv()


def backward(layer, e_seq, gates, c_seq, w_stack, steps):
    n, hidden = e_seq.shape
    width = 4 * hidden
    rows = n // steps
    last = steps - 1
    anywhere = pl.BlockSpec(memory_space=pl.ANY)
    return pl.pallas_call(
        functools.partial(backward_kernel, layer, steps, rows, hidden),
        grid=(steps,),
        in_specs=[
            pl.BlockSpec((rows, hidden), lambda s: (last - s, 0)),
            pl.BlockSpec((rows, width), lambda s: (last - s, 0)),
            pl.BlockSpec((rows, hidden), lambda s: (last - s, 0)),
            pl.BlockSpec((rows, hidden), lambda s: (jnp.maximum(last - 1 - s, 0), 0)),
            anywhere,
        ],
        out_specs=[anywhere, pl.BlockSpec((n, hidden), lambda s: (0, 0))],
        out_shape=[
            jax.ShapeDtypeStruct((PEERS, n + EXTRA, width // PEERS), jnp.bfloat16),
            jax.ShapeDtypeStruct((n, hidden), jnp.float32),
        ],
        scratch_shapes=[
            pltpu.VMEM((rows, hidden), jnp.float32),
            pltpu.VMEM((rows, hidden), jnp.float32),
            pltpu.VMEM((1, width), jnp.float32),
            pltpu.VMEM((n + EXTRA, width), jnp.bfloat16),
            pltpu.VMEM((hidden, width), jnp.bfloat16),
            pltpu.VMEM((hidden, width), jnp.bfloat16),
            pltpu.SemaphoreType.DMA((2,)),
            pltpu.SemaphoreType.DMA,
            pltpu.SemaphoreType.DMA((PEERS,)),
            pltpu.SemaphoreType.DMA((PEERS,)),
        ],
        compiler_params=pltpu.CompilerParams(vmem_limit_bytes=VMEM_LIMIT, collective_id=layer, has_side_effects=True),
        cost_estimate=pl.CostEstimate(flops=2 * n * 2 * hidden * width * 4, bytes_accessed=2 * 2 * hidden * width, transcendentals=0),
        name="lstm_backward",
    )(e_seq, gates, c_seq, c_seq, w_stack)


def weight_kernel(n, rows, hidden, land_ref, u_own, u_other, h_own, h_other, *refs):
    *out_refs, acc, db_acc, dz_t = refs
    s = pl.program_id(0)
    share = land_ref.shape[-1]

    @pl.when(s == 0)
    def _():
        acc[...] = jnp.zeros_like(acc)
        db_acc[...] = jnp.zeros_like(db_acc)

    db_acc[...] += land_ref[0, pl.ds(n, EXTRA), :].astype(jnp.float32)
    dz_t[...] = land_ref[0, pl.ds(0, n), :].T
    part = 256

    def add(u_ref, h_ref):
        @pl.loop(0, hidden // part)
        def _(p):
            rc = pl.ds(pl.multiple_of(p * part, part), part)
            hc = pl.ds(pl.multiple_of(hidden + p * part, part), part)
            h_prev = jnp.concatenate([jnp.zeros((rows, part), jnp.bfloat16), h_ref[0, pl.ds(0, n - rows), rc]], axis=0)
            for cols, rhs in ((rc, u_ref[0, :, rc]), (hc, h_prev)):
                dw = jnp.dot(dz_t[...], rhs, preferred_element_type=jnp.float32)
                acc[:, cols] += dw.astype(jnp.bfloat16).astype(jnp.float32)

    @pl.when(s < CHIPS)
    def _():
        add(u_own, h_own)

    @pl.when(s >= CHIPS)
    def _():
        add(u_other, h_other)

    @pl.when(s == PEERS - 1)
    def _():
        height = 2 * hidden // len(out_refs)
        for half, out_ref in enumerate(out_refs):
            @pl.loop(0, height // part)
            def _(p):
                cols = pl.ds(pl.multiple_of(half * height + p * part, part), part)
                out_ref[pl.ds(pl.multiple_of(p * part, part), part), :] = acc[:, cols].T.astype(jnp.bfloat16)

        out_refs[-1][pl.ds(height, EXTRA), :] = db_acc[...].astype(jnp.bfloat16)


def weight_gradient(land, u_all, h_all, rows, pieces):
    _, height, share = land.shape
    _, n, hidden = u_all[0].shape
    heights = [2 * hidden // pieces] * (pieces - 1) + [2 * hidden // pieces + EXTRA]
    own = pl.BlockSpec((1, n, hidden), lambda s: (jnp.minimum(s, CHIPS - 1), 0, 0))
    other = pl.BlockSpec((1, n, hidden), lambda s: (jnp.maximum(s - CHIPS, 0), 0, 0))
    return pl.pallas_call(
        functools.partial(weight_kernel, n, rows, hidden),
        grid=(PEERS,),
        in_specs=[pl.BlockSpec((1, height, share), lambda s: (s, 0, 0)), own, other, own, other],
        out_specs=[pl.BlockSpec((h, share), lambda s: (0, 0)) for h in heights],
        out_shape=[jax.ShapeDtypeStruct((h, share), jnp.bfloat16) for h in heights],
        scratch_shapes=[
            pltpu.VMEM((share, 2 * hidden), jnp.float32),
            pltpu.VMEM((EXTRA, share), jnp.float32),
            pltpu.VMEM((share, n), jnp.bfloat16),
        ],
        compiler_params=pltpu.CompilerParams(vmem_limit_bytes=VMEM_LIMIT),
        cost_estimate=pl.CostEstimate(flops=2 * PEERS * n * share * 2 * hidden * 4, bytes_accessed=4 * PEERS * n * hidden, transcendentals=0),
        name="weight_gradient",
    )(land, *u_all, *h_all)


def cast_kernel(with_db, core_ref, own_ref, other_ref, *refs):
    core = core_ref[0]
    share = own_ref.shape[-1]
    out_ref = refs[-2] if with_db else refs[-1]
    for chip in range(CHIPS):
        for i, (which, src) in enumerate(((core, own_ref), (1 - core, other_ref))):
            cols = pl.ds(pl.multiple_of((chip * 2 + which) * share, share), share)
            out_ref[0, :, cols] = src[chip].astype(jnp.float32)
            if with_db:
                refs[-1][0, :, cols] = refs[i][chip, pl.ds(0, 8), :][0:1].astype(jnp.float32)


def cast_into(bufs, core, parts, layer, layers, first, hidden):
    _, height, share = parts[0].shape
    with_db = height % 128 != 0
    height -= EXTRA if with_db else 0
    tile = 128
    width = PEERS * share
    big = pl.BlockSpec((CHIPS, tile, share), lambda i: (0, i, 0))
    small = pl.BlockSpec((CHIPS, EXTRA, share), lambda i: (0, height // EXTRA, 0))
    outs = 2 if with_db else 1
    bufs = list(bufs)
    operands = [core, *parts] + (list(parts) if with_db else [])
    dw_db = pl.pallas_call(
        functools.partial(cast_kernel, with_db),
        grid=(height // tile,),
        in_specs=[pl.BlockSpec(memory_space=pltpu.SMEM), big, big] + [small] * (len(operands) - 3) + [pl.BlockSpec(memory_space=pl.ANY)] * (outs if bufs else 0),
        out_specs=[pl.BlockSpec((1, tile, width), lambda i: (layer, first // tile + i, 0)), pl.BlockSpec((1, 1, width), lambda i: (layer, 0, 0))][:outs],
        out_shape=[jax.ShapeDtypeStruct((layers, 2 * hidden, width), jnp.float32), jax.ShapeDtypeStruct((layers, 1, width), jnp.float32)][:outs],
        input_output_aliases={len(operands) + k: k for k in range(outs)} if bufs else {},
        compiler_params=pltpu.CompilerParams(vmem_limit_bytes=VMEM_LIMIT),
        cost_estimate=pl.CostEstimate(flops=height * width * 100, bytes_accessed=6 * height * width, transcendentals=0),
        name="cast_gradient",
    )(*operands, *bufs[:outs])
    return list(dw_db) + bufs[outs:]


def solution(mesh):
    batch_axes = ('replica', 'data')
    swap = [(0, 1), (1, 0)]

    def tie(*values):
        return lax.optimization_barrier(values)

    def local_grads(x_loc, dy_loc, w_stack, b_stack):
        layers = w_stack.shape[0]
        rows, steps, hidden = x_loc.shape
        n = rows * steps
        core = lax.axis_index('data').astype(jnp.int32).reshape(1)
        u = jnp.swapaxes(x_loc, 0, 1).reshape(n, hidden)
        b_rows = b_stack[:, None, :]
        own = []
        other = []
        saved = []
        for layer in range(layers):
            own.append(lax.all_gather(u, 'replica'))
            if layer >= 2:
                u, own[layer - 2] = tie(u, own[layer - 2])
                other.append(lax.ppermute(own[layer - 2], 'data', swap))
            if layer >= 3:
                u, other[layer - 3] = tie(u, other[layer - 3])
            gates, c_seq, u = forward(layer, u, w_stack, b_rows, steps)
            saved.append((gates, c_seq))
        own.append(lax.all_gather(u, 'replica'))
        e_seq = jnp.swapaxes(dy_loc, 0, 1).reshape(n, hidden)
        e_seq, own[layers - 2], other[layers - 3] = tie(e_seq, own[layers - 2], other[layers - 3])
        other.append(lax.ppermute(own[layers - 2], 'data', swap))
        bufs = []
        shard = None
        pending = None
        for layer in reversed(range(layers)):
            land, e_seq = backward(layer, e_seq, *saved[layer], w_stack, steps)
            if layer == layers - 1:
                land, own[layers - 1], own[layers] = tie(land, own[layers - 1], own[layers])
                other.append(lax.ppermute(own[layers - 1], 'data', swap))
                other.append(lax.ppermute(own[layers], 'data', swap))
            if pending is not None:
                done_own, done_other, e_seq = tie(*pending, e_seq)
                bufs = cast_into(bufs, core, (done_own, done_other), layer + 2, layers, 0, hidden)
            parts = weight_gradient(land, (own[layer], other[layer]), (own[layer + 1], other[layer + 1]), rows, 1 if layer else 2)
            *parts, e_seq = tie(*parts, e_seq)
            if shard is not None:
                *parts, shard = tie(*parts, shard)
                if bufs:
                    parts[0], bufs[1] = tie(parts[0], bufs[1])
                pending = (shard, lax.ppermute(shard, 'data', swap))
            shard = lax.all_gather(parts[0], 'replica')
        bufs = cast_into(bufs, core, pending, 1, layers, 0, hidden)
        dx = jnp.swapaxes(e_seq.reshape(steps, rows, hidden), 0, 1)
        top, bottom, dx, bufs[1] = tie(shard, parts[1], dx, bufs[1])
        bottom = lax.all_gather(bottom, 'replica')
        bufs = cast_into(bufs, core, (top, lax.ppermute(top, 'data', swap)), 0, layers, 0, hidden)
        bottom, bufs[0] = tie(bottom, bufs[0])
        dw, db = cast_into(bufs, core, (bottom, lax.ppermute(bottom, 'data', swap)), 0, layers, hidden, hidden)
        return dw, db.reshape(layers, 4 * hidden), dx

    return jax.shard_map(local_grads, mesh=mesh, in_specs=(P(batch_axes), P(batch_axes), P(), P()), out_specs=(P(), P(), P(batch_axes)), check_vma=False)
```

```python
import functools

import jax
import jax.numpy as jnp
from jax import lax
from jax.experimental import pallas as pl
from jax.experimental.pallas import tpu as pltpu
from jax.sharding import PartitionSpec as P

VMEM_LIMIT = 62 * 1024 * 1024
CHIPS = 4
PEERS = 8
EXTRA = 16
NT = (((1,), (1,)), ((), ()))
MESH = pl.DeviceIdType.MESH


def sigmoid(z):
    return 0.5 * jnp.tanh(0.5 * z) + 0.5


def forward_kernel(layer, steps, rows, hidden, u_ref, w_hbm, b_ref, gates_hbm, c_hbm, h_ref, w_in, w_rec, gates, c_buf, w_sem, out_sem):
    tile = 512
    tiles = 4 * hidden // tile

    def in_copy(j):
        cols = pl.ds(j * tile, tile)
        return pltpu.make_async_copy(w_hbm.at[layer, pl.ds(0, hidden), cols], w_in.at[:, cols], w_sem.at[j])

    for j in range(tiles):
        in_copy(j).start()
    rec_copy = pltpu.make_async_copy(w_hbm.at[layer, pl.ds(hidden, hidden)], w_rec, w_sem.at[tiles])
    rec_copy.start()
    for j in range(tiles):
        cols = pl.ds(j * tile, tile)
        in_copy(j).wait()
        gates[:, cols] = jnp.dot(u_ref[...], w_in[:, cols], preferred_element_type=jnp.float32) + b_ref[0, :, cols]
    rec_copy.wait()
    part = 256

    def out_copies(t):
        r = pl.ds(pl.multiple_of(t * rows, rows), rows)
        return (pltpu.make_async_copy(gates.at[r], gates_hbm.at[r], out_sem.at[0]), pltpu.make_async_copy(c_buf.at[r], c_hbm.at[r], out_sem.at[1]))

    def step(t, first):
        r = pl.ds(pl.multiple_of(t * rows, rows), rows)
        if not first:
            rp = pl.ds(pl.multiple_of((t - 1) * rows, rows), rows)
            h_prev = h_ref[rp, :]
            for copy in out_copies(t - 1):
                copy.start()
        for p in range(hidden // part):
            z = []
            for k in range(4):
                cols = pl.ds(k * hidden + p * part, part)
                zk = gates[r, cols]
                if not first:
                    zk = zk + jnp.dot(h_prev, w_rec[:, cols], preferred_element_type=jnp.float32)
                z.append(zk)
            pc = pl.ds(p * part, part)
            gate_i, gate_f, gate_g, gate_o = sigmoid(z[0]), sigmoid(z[1]), jnp.tanh(z[2]), sigmoid(z[3])
            c_new = gate_i * gate_g
            if not first:
                c_new = gate_f * c_buf[rp, pc] + c_new
            for k, v in enumerate((gate_i, gate_f, gate_g, gate_o)):
                gates[r, pl.ds(k * hidden + p * part, part)] = v
            c_buf[r, pc] = c_new
            h_ref[r, pc] = (gate_o * jnp.tanh(c_new)).astype(jnp.bfloat16)

    step(0, True)

    @pl.loop(1, steps)
    def _(t):
        step(t, False)

    for copy in out_copies(steps - 1):
        copy.start()
    pltpu.make_async_copy(gates, gates_hbm, out_sem.at[0]).wait()
    pltpu.make_async_copy(c_buf, c_hbm, out_sem.at[1]).wait()


def forward(layer, u, w_stack, b_stack, steps):
    n, hidden = u.shape
    width = 4 * hidden
    whole = pl.BlockSpec(memory_space=pltpu.VMEM)
    anywhere = pl.BlockSpec(memory_space=pl.ANY)
    return pl.pallas_call(
        functools.partial(forward_kernel, layer, steps, n // steps, hidden),
        grid=(1,),
        in_specs=[
            pl.BlockSpec((n, hidden), lambda i: (0, 0)),
            anywhere,
            pl.BlockSpec((1, 1, width), lambda i: (layer, 0, 0)),
        ],
        out_specs=[anywhere, anywhere, pl.BlockSpec((n, hidden), lambda i: (0, 0))],
        out_shape=[
            jax.ShapeDtypeStruct((n, width), jnp.float32),
            jax.ShapeDtypeStruct((n, hidden), jnp.float32),
            jax.ShapeDtypeStruct((n, hidden), jnp.bfloat16),
        ],
        scratch_shapes=[
            pltpu.VMEM((hidden, width), jnp.bfloat16),
            pltpu.VMEM((hidden, width), jnp.bfloat16),
            pltpu.VMEM((n, width), jnp.float32),
            pltpu.VMEM((n, hidden), jnp.float32),
            pltpu.SemaphoreType.DMA((9,)),
            pltpu.SemaphoreType.DMA((2,)),
        ],
        compiler_params=pltpu.CompilerParams(vmem_limit_bytes=VMEM_LIMIT),
        cost_estimate=pl.CostEstimate(flops=2 * n * 2 * hidden * width * 4, bytes_accessed=2 * 2 * hidden * width, transcendentals=0),
        name="lstm_forward",
    )(u, w_stack, b_stack)


def backward_kernel(layer, steps, rows, hidden, e_ref, gates_ref, c_ref, cp_ref, w_hbm, land, dx_ref, r_buf, dc_buf, db_buf, dz_buf, w_in, w_rec, w_sem, own_sem, send_sem, recv_sem):
    s = pl.program_id(0)
    t = steps - 1 - s
    width = 4 * hidden
    share = width // PEERS
    n = steps * rows
    chip = lax.axis_index("replica")
    core = lax.axis_index("data")
    chips = (chip, chip + 1 - 2 * lax.rem(chip, 2), lax.rem(chip + 2, 4), 3 - chip)
    cores = (core, 1 - core)
    rec_copy = pltpu.make_async_copy(w_hbm.at[layer, pl.ds(hidden, hidden)], w_rec, w_sem.at[0])
    in_copy = pltpu.make_async_copy(w_hbm.at[layer, pl.ds(0, hidden)], w_in, w_sem.at[1])

    def own_copy(start, count):
        r = pl.ds(start, count)
        cols = pl.ds(pl.multiple_of((chip * 2 + core) * share, share), share)
        return pltpu.make_async_copy(dz_buf.at[r, cols], land.at[chip, r], own_sem)

    def send_copy(k, start, count):
        to_chip, to_core = chips[k % 4], cores[k // 4]
        r = pl.ds(start, count)
        cols = pl.ds(pl.multiple_of((to_chip * 2 + to_core) * share, share), share)
        return pltpu.make_async_remote_copy(
            src_ref=dz_buf.at[r, cols],
            dst_ref=land.at[chip + 4 * (k // 4), r],
            send_sem=send_sem.at[k],
            recv_sem=recv_sem.at[k],
            device_id=(to_chip, to_core),
            device_id_type=MESH,
        )

    def send(start, count):
        for k in (3, 7, 1, 2, 5, 6, 4):
            send_copy(k, start, count).start()
        own_copy(start, count).start()

    @pl.when(s == 0)
    def _():
        rec_copy.start()
        in_copy.start()
        barrier = pltpu.get_barrier_semaphore()
        for k in range(1, PEERS):
            pl.semaphore_signal(barrier, inc=1, device_id=(chips[k % 4], cores[k // 4]), device_id_type=MESH)
        r_buf[...] = jnp.zeros_like(r_buf)
        dc_buf[...] = jnp.zeros_like(dc_buf)
        db_buf[...] = jnp.zeros_like(db_buf)
        rec_copy.wait()
        pl.semaphore_wait(barrier, PEERS - 1)

    for q in range(1, 4):
        @pl.when(s == 4 * q)
        def _():
            send(n - 4 * q * rows, 4 * rows)

    @pl.when(s == steps - 1)
    def _():
        send(rows, 3 * rows)

    keep = jnp.where(t == 0, 0.0, 1.0)
    part = 256
    for p in range(hidden // part):
        pc = pl.ds(p * part, part)
        gate_i, gate_f, gate_g, gate_o = (gates_ref[:, pl.ds(k * hidden + p * part, part)] for k in range(4))
        tanh_c = jnp.tanh(c_ref[:, pc])
        c_prev = cp_ref[:, pc] * keep
        dh = e_ref[:, pc] + r_buf[:, pc]
        dc = dc_buf[:, pc] + dh * gate_o * (1.0 - tanh_c * tanh_c)
        dz = (
            dc * gate_g * gate_i * (1.0 - gate_i),
            dc * c_prev * gate_f * (1.0 - gate_f),
            dc * gate_i * (1.0 - gate_g * gate_g),
            dh * tanh_c * gate_o * (1.0 - gate_o),
        )
        dc_buf[:, pc] = dc * gate_f
        for k in range(4):
            cols = pl.ds(k * hidden + p * part, part)
            dz_buf[pl.ds(pl.multiple_of(t * rows, rows), rows), cols] = dz[k].astype(jnp.bfloat16)
            db_buf[:, cols] += jnp.sum(dz[k], axis=0, keepdims=True)

    @pl.when(s < steps - 1)
    def _():
        low = dz_buf[pl.ds(pl.multiple_of(t * rows, rows), rows), :]
        for p in range(hidden // part):
            pc = pl.ds(p * part, part)
            r_buf[:, pc] = lax.dot_general(low, w_rec[pc, :], NT, preferred_element_type=jnp.float32)

    @pl.when(s == steps - 1)
    def _():
        dz_buf[pl.ds(n, EXTRA), :] = jnp.broadcast_to(db_buf[...], (EXTRA, width)).astype(jnp.bfloat16)
        in_copy.wait()

        def dx_tile(p):
            pc = pl.ds(pl.multiple_of(p * part, part), part)
            dx_ref[:, pc] = lax.dot_general(dz_buf[pl.ds(0, n), :], w_in[pc, :], NT, preferred_element_type=jnp.float32)

        @pl.loop(0, 1)
        def _(p):
            dx_tile(p)

        send(0, rows)
        send(n, EXTRA)

        @pl.loop(1, hidden // part)
        def _(p):
            dx_tile(p)

        own_copy(0, n + EXTRA).wait()
        for k in range(1, PEERS):
            send_copy(k, 0, n + EXTRA).wait_send()
            cols = pl.ds(pl.multiple_of((chip * 2 + core) * share, share), share)
            pltpu.make_async_remote_copy(
                src_ref=dz_buf.at[:, cols],
                dst_ref=land.at[chips[k % 4] + 4 * (k // 4)],
                send_sem=send_sem.at[k],
                recv_sem=recv_sem.at[k],
                device_id=(chips[k % 4], cores[k // 4]),
                device_id_type=MESH,
            ).wait_recv()


def backward(layer, e_seq, gates, c_seq, w_stack, steps):
    n, hidden = e_seq.shape
    width = 4 * hidden
    rows = n // steps
    last = steps - 1
    anywhere = pl.BlockSpec(memory_space=pl.ANY)
    return pl.pallas_call(
        functools.partial(backward_kernel, layer, steps, rows, hidden),
        grid=(steps,),
        in_specs=[
            pl.BlockSpec((rows, hidden), lambda s: (last - s, 0)),
            pl.BlockSpec((rows, width), lambda s: (last - s, 0)),
            pl.BlockSpec((rows, hidden), lambda s: (last - s, 0)),
            pl.BlockSpec((rows, hidden), lambda s: (jnp.maximum(last - 1 - s, 0), 0)),
            anywhere,
        ],
        out_specs=[anywhere, pl.BlockSpec((n, hidden), lambda s: (0, 0))],
        out_shape=[
            jax.ShapeDtypeStruct((PEERS, n + EXTRA, width // PEERS), jnp.bfloat16),
            jax.ShapeDtypeStruct((n, hidden), jnp.float32),
        ],
        scratch_shapes=[
            pltpu.VMEM((rows, hidden), jnp.float32),
            pltpu.VMEM((rows, hidden), jnp.float32),
            pltpu.VMEM((1, width), jnp.float32),
            pltpu.VMEM((n + EXTRA, width), jnp.bfloat16),
            pltpu.VMEM((hidden, width), jnp.bfloat16),
            pltpu.VMEM((hidden, width), jnp.bfloat16),
            pltpu.SemaphoreType.DMA((2,)),
            pltpu.SemaphoreType.DMA,
            pltpu.SemaphoreType.DMA((PEERS,)),
            pltpu.SemaphoreType.DMA((PEERS,)),
        ],
        compiler_params=pltpu.CompilerParams(vmem_limit_bytes=VMEM_LIMIT, collective_id=layer, has_side_effects=True),
        cost_estimate=pl.CostEstimate(flops=2 * n * 2 * hidden * width * 4, bytes_accessed=2 * 2 * hidden * width, transcendentals=0),
        name="lstm_backward",
    )(e_seq, gates, c_seq, c_seq, w_stack)


def weight_kernel(n, rows, hidden, land_ref, u_own, u_other, h_own, h_other, *refs):
    *out_refs, acc, db_acc, dz_t = refs
    s = pl.program_id(0)
    share = land_ref.shape[-1]

    @pl.when(s == 0)
    def _():
        acc[...] = jnp.zeros_like(acc)
        db_acc[...] = jnp.zeros_like(db_acc)

    db_acc[...] += land_ref[0, pl.ds(n, EXTRA), :].astype(jnp.float32)
    dz_t[...] = land_ref[0, pl.ds(0, n), :].T
    part = 256

    def add(u_ref, h_ref):
        for p in range(hidden // part):
            rc = pl.ds(p * part, part)
            hc = pl.ds(hidden + p * part, part)
            h_prev = jnp.concatenate([jnp.zeros((rows, part), jnp.bfloat16), h_ref[0, pl.ds(0, n - rows), rc]], axis=0)
            for cols, rhs in ((rc, u_ref[0, :, rc]), (hc, h_prev)):
                dw = jnp.dot(dz_t[...], rhs, preferred_element_type=jnp.float32)
                acc[:, cols] += dw.astype(jnp.bfloat16).astype(jnp.float32)

    @pl.when(s < CHIPS)
    def _():
        add(u_own, h_own)

    @pl.when(s >= CHIPS)
    def _():
        add(u_other, h_other)

    @pl.when(s == PEERS - 1)
    def _():
        height = 2 * hidden // len(out_refs)
        for half, out_ref in enumerate(out_refs):
            @pl.loop(0, height // part)
            def _(p):
                cols = pl.ds(pl.multiple_of(half * height + p * part, part), part)
                out_ref[pl.ds(pl.multiple_of(p * part, part), part), :] = acc[:, cols].astype(jnp.bfloat16).T

        out_refs[-1][pl.ds(height, EXTRA), :] = db_acc[...].astype(jnp.bfloat16)


def weight_gradient(land, u_all, h_all, rows, pieces):
    _, height, share = land.shape
    _, n, hidden = u_all[0].shape
    heights = [2 * hidden // pieces] * (pieces - 1) + [2 * hidden // pieces + EXTRA]
    own = pl.BlockSpec((1, n, hidden), lambda s: (jnp.minimum(s, CHIPS - 1), 0, 0))
    other = pl.BlockSpec((1, n, hidden), lambda s: (jnp.maximum(s - CHIPS, 0), 0, 0))
    return pl.pallas_call(
        functools.partial(weight_kernel, n, rows, hidden),
        grid=(PEERS,),
        in_specs=[pl.BlockSpec((1, height, share), lambda s: (s, 0, 0)), own, other, own, other],
        out_specs=[pl.BlockSpec((h, share), lambda s: (0, 0)) for h in heights],
        out_shape=[jax.ShapeDtypeStruct((h, share), jnp.bfloat16) for h in heights],
        scratch_shapes=[
            pltpu.VMEM((share, 2 * hidden), jnp.float32),
            pltpu.VMEM((EXTRA, share), jnp.float32),
            pltpu.VMEM((share, n), jnp.bfloat16),
        ],
        compiler_params=pltpu.CompilerParams(vmem_limit_bytes=VMEM_LIMIT),
        cost_estimate=pl.CostEstimate(flops=2 * PEERS * n * share * 2 * hidden * 4, bytes_accessed=4 * PEERS * n * hidden, transcendentals=0),
        name="weight_gradient",
    )(land, *u_all, *h_all)


def cast_kernel(with_db, core_ref, own_ref, other_ref, *refs):
    core = core_ref[0]
    share = own_ref.shape[-1]
    out_ref = refs[-2] if with_db else refs[-1]
    for chip in range(CHIPS):
        for i, (which, src) in enumerate(((core, own_ref), (1 - core, other_ref))):
            cols = pl.ds(pl.multiple_of((chip * 2 + which) * share, share), share)
            out_ref[0, :, cols] = src[chip].astype(jnp.float32)
            if with_db:
                refs[-1][0, :, cols] = refs[i][chip, pl.ds(0, 8), :][0:1].astype(jnp.float32)


def cast_into(bufs, core, parts, layer, layers, first, hidden):
    _, height, share = parts[0].shape
    with_db = height % 128 != 0
    height -= EXTRA if with_db else 0
    tile = 128
    width = PEERS * share
    big = pl.BlockSpec((CHIPS, tile, share), lambda i: (0, i, 0))
    small = pl.BlockSpec((CHIPS, EXTRA, share), lambda i: (0, height // EXTRA, 0))
    outs = 2 if with_db else 1
    bufs = list(bufs)
    operands = [core, *parts] + (list(parts) if with_db else [])
    dw_db = pl.pallas_call(
        functools.partial(cast_kernel, with_db),
        grid=(height // tile,),
        in_specs=[pl.BlockSpec(memory_space=pltpu.SMEM), big, big] + [small] * (len(operands) - 3) + [pl.BlockSpec(memory_space=pl.ANY)] * (outs if bufs else 0),
        out_specs=[pl.BlockSpec((1, tile, width), lambda i: (layer, first // tile + i, 0)), pl.BlockSpec((1, 1, width), lambda i: (layer, 0, 0))][:outs],
        out_shape=[jax.ShapeDtypeStruct((layers, 2 * hidden, width), jnp.float32), jax.ShapeDtypeStruct((layers, 1, width), jnp.float32)][:outs],
        input_output_aliases={len(operands) + k: k for k in range(outs)} if bufs else {},
        compiler_params=pltpu.CompilerParams(vmem_limit_bytes=VMEM_LIMIT),
        cost_estimate=pl.CostEstimate(flops=height * width * 100, bytes_accessed=6 * height * width, transcendentals=0),
        name="cast_gradient",
    )(*operands, *bufs[:outs])
    return list(dw_db) + bufs[outs:]


def solution(mesh):
    batch_axes = ('replica', 'data')
    swap = [(0, 1), (1, 0)]

    def tie(*values):
        return lax.optimization_barrier(values)

    def local_grads(x_loc, dy_loc, w_stack, b_stack):
        layers = w_stack.shape[0]
        rows, steps, hidden = x_loc.shape
        n = rows * steps
        core = lax.axis_index('data').astype(jnp.int32).reshape(1)
        u = jnp.swapaxes(x_loc, 0, 1).reshape(n, hidden)
        b_rows = b_stack[:, None, :]
        own = []
        other = []
        saved = []
        for layer in range(layers):
            own.append(lax.all_gather(u, 'replica'))
            if layer >= 3:
                u, own[layer - 3] = tie(u, own[layer - 3])
                other.append(lax.ppermute(own[layer - 3], 'data', swap))
            if layer >= 4:
                u, other[layer - 4] = tie(u, other[layer - 4])
            gates, c_seq, u = forward(layer, u, w_stack, b_rows, steps)
            saved.append((gates, c_seq))
        own.append(lax.all_gather(u, 'replica'))
        e_seq = jnp.swapaxes(dy_loc, 0, 1).reshape(n, hidden)
        e_seq, own[layers - 3], other[layers - 4] = tie(e_seq, own[layers - 3], other[layers - 4])
        other.append(lax.ppermute(own[layers - 3], 'data', swap))
        bufs = []
        shard = None
        pending = None
        for layer in reversed(range(layers)):
            land, e_seq = backward(layer, e_seq, *saved[layer], w_stack, steps)
            if layer == layers - 1:
                land, own[layers - 2], own[layers - 1], own[layers] = tie(land, own[layers - 2], own[layers - 1], own[layers])
                other.append(lax.ppermute(own[layers - 2], 'data', swap))
                other.append(lax.ppermute(own[layers - 1], 'data', swap))
                other.append(lax.ppermute(own[layers], 'data', swap))
            if pending is not None:
                done_own, done_other, e_seq = tie(*pending, e_seq)
                bufs = cast_into(bufs, core, (done_own, done_other), layer + 2, layers, 0, hidden)
            parts = weight_gradient(land, (own[layer], other[layer]), (own[layer + 1], other[layer + 1]), rows, 1 if layer else 2)
            *parts, e_seq = tie(*parts, e_seq)
            if shard is not None:
                *parts, shard = tie(*parts, shard)
                if bufs and layer:
                    parts[0], bufs[1] = tie(parts[0], bufs[1])
                pending = (shard, lax.ppermute(shard, 'data', swap))
            shard = lax.all_gather(parts[0], 'replica')
        bufs = cast_into(bufs, core, pending, 1, layers, 0, hidden)
        dx = jnp.swapaxes(e_seq.reshape(steps, rows, hidden), 0, 1)
        top, bottom, dx, bufs[1] = tie(shard, parts[1], dx, bufs[1])
        bottom = lax.all_gather(bottom, 'replica')
        bufs = cast_into(bufs, core, (top, lax.ppermute(top, 'data', swap)), 0, layers, 0, hidden)
        bottom, bufs[0] = tie(bottom, bufs[0])
        dw, db = cast_into(bufs, core, (bottom, lax.ppermute(bottom, 'data', swap)), 0, layers, hidden, hidden)
        return dw, db.reshape(layers, 4 * hidden), dx

    return jax.shard_map(local_grads, mesh=mesh, in_specs=(P(batch_axes), P(batch_axes), P(), P()), out_specs=(P(), P(), P(batch_axes)), check_vma=False)
```
